32 devices in a mesh: grp: 2 (over y), ia: 4 (over z), ja: 4 (over x, core).
Axes of the slice: x: 2, y: 2, z: 4, core: 2. Of those that a mesh axis runs over, the one named last changes fastest.
Arguments:
- doubles: bfloat16 [8, 16, 384, 384], P(('grp', 'ia'), 'ja'), parts along dimension 0, may hold values from -6 to 6
- aux_factors: bfloat16 [4, 384, 384], P('ia'), may hold values from -0.15625 to 0.15625
- cycle_factors: bfloat16 [16, 384, 128], replicated, may hold values from -0.21875 to 0.21875
Outputs:
- sigma: bfloat16 [8, 16, 384, 384], P(('grp', 'ia'), 'ja'), parts along dimension 0
The draws below stay inside these ranges and needn't reach their ends.
There are 2 independent parts, one for each index of `grp`. The reference program is written for one: setup_inputs(seed, part) draws one part's arguments, and reference() takes and returns one part's arrays. A program takes and returns all parts, laid end to end along the dimension named above; an argument that names none is the same for every part. Nothing has to cross between parts.
All inputs are finite; a program needn't handle non-finite values.
Results may differ from the reference program's by a relative error of at most 0.008.
Values may be sent and summed in bfloat16 or wider, within the bound.
A program may use at most 128 MiB of HBM per device.

```python
import jax
import jax.numpy as jnp
from jax import lax

V = 384
Q = 128
AUX = 4
OI = 4
J_ALL = 16


def block_scale(rng, dims, split, low, high):
    loudness = 1.0
    for dim, shards_of in split:
        draws = jax.random.uniform(jax.random.fold_in(jax.random.fold_in(rng, 6), dim), (shards_of,), jnp.float32, low / len(split), high / len(split))
        loudness = loudness * jnp.repeat(jnp.exp(draws), dims[dim] // shards_of).reshape((-1,) + (1,) * (len(dims) - 1 - dim))
    return loudness


def noise(own_key, dims, spread, reach, shards=(), held_as=jnp.bfloat16):
    result = jax.random.normal(own_key, dims, jnp.float32) * spread
    if len(shards) > 0:
        result = block_scale(own_key, dims, shards, -0.22, 0.18) * result
    return jnp.clip(result, min=-reach, max=reach).astype(held_as)


def setup_inputs(seed: int = 0, part: int = 0) -> dict:
    streams_of = jax.random.split(jax.random.key(seed), 4)
    own_keys = jax.random.split(jax.random.fold_in(streams_of[3], part), 4)
    doubles = noise(own_keys[0], (OI, J_ALL, V, V), 1.0, 6.0, ((0, 4), (1, 4)))
    aux_factors = noise(streams_of[1], (AUX, V, V), (V * 4) ** -0.5, 0.15625, ((0, 4),))
    cycle_factors = noise(streams_of[2], (J_ALL, V, Q), (J_ALL * V // 8) ** -0.5, 0.21875)
    return dict(doubles=doubles, aux_factors=aux_factors, cycle_factors=cycle_factors)


def ladder_terms(pair_blocks, factor):
    wide_pairs = pair_blocks.astype(jnp.float32)
    wide_factor = factor.astype(jnp.float32)
    halfway = jnp.einsum('pcd,bd->pcb', wide_pairs, wide_factor).astype(jnp.bfloat16)
    return jnp.einsum('ac,pcb->pab', wide_factor, halfway.astype(jnp.float32))


def reference(doubles, aux_factors, cycle_factors):
    pair_blocks = doubles.reshape(OI * J_ALL, V, V)

    def one_step(position, running):
        factor = lax.dynamic_index_in_dim(aux_factors, position, 0, keepdims=False)
        return running + ladder_terms(pair_blocks, factor)

    ladder = lax.fori_loop(0, AUX, one_step, jnp.zeros((OI * J_ALL, V, V), jnp.float32))
    ladder = ladder.reshape(OI, J_ALL, V, V)
    wide_cycle = cycle_factors.astype(jnp.float32)
    latent = jnp.einsum('ijab,jbq->iaq', doubles.astype(jnp.float32), wide_cycle).astype(jnp.bfloat16)
    cycle_term = jnp.einsum('iaq,jbq->ijab', latent.astype(jnp.float32), wide_cycle).astype(jnp.bfloat16)
    return (ladder + cycle_term.astype(jnp.float32)).astype(jnp.bfloat16)
```

```python
import functools

import jax
import jax.numpy as jnp
from jax import lax
from jax.experimental import pallas as pl
from jax.experimental.pallas import tpu as pltpu
from jax.sharding import PartitionSpec as P

MESH = pl.DeviceIdType.MESH
F32 = jnp.float32
BF16 = jnp.bfloat16
NT = (((1,), (1,)), ((), ()))
CORES = 2


def sigma_kernel(n, nj, d_hbm, aux_hbm, u_hbm, out_hbm, d, u, aux, half, acc, out,
                 plat, lat_in, lat, load_sem, out_sem, z_send, z_recv, x_send, x_recv,
                 s_send, s_recv, p_send, p_recv, l_send, l_recv):
    nx = nj // CORES
    pairs_j, width = d.shape[0], d.shape[1]
    grp_j = half.shape[2] // width
    n_jp = pairs_j // grp_j
    rows = width // nj
    iz = lax.axis_index("ia")
    ij = lax.axis_index("ja")
    sibling = ij ^ 1

    def chunk(owner):
        return pl.ds(pl.multiple_of(owner * rows, rows), rows)

    def slot(k):
        return pl.ds(k * width, width)

    load_aux = pltpu.make_async_copy(aux_hbm.at[0], aux.at[:, slot(0)], load_sem.at[0])
    load_d = pltpu.make_async_copy(d_hbm.at[0], d, load_sem.at[1])
    load_u = pltpu.make_async_copy(
        u_hbm.at[pl.ds(ij * pairs_j, pairs_j)], u, load_sem.at[2])
    load_aux.start()
    load_d.start()
    load_u.start()

    barrier = pltpu.get_barrier_semaphore()
    for k in range(1, n):
        pl.semaphore_signal(barrier, inc=1, device_id={"ia": iz ^ k}, device_id_type=MESH)
    for m in range(1, nj):
        pl.semaphore_signal(barrier, inc=1, device_id={"ja": ij ^ m}, device_id_type=MESH)
    pl.semaphore_wait(barrier, n - 1 + nj - 1)

    def remote(src, dst, send, recv, where):
        return pltpu.make_async_remote_copy(
            src_ref=src, dst_ref=dst, send_sem=send, recv_sem=recv,
            device_id=where, device_id_type=MESH)

    def z_copy(k):
        return remote(aux.at[chunk(ij), slot(0)], aux.at[chunk(ij), slot(k)],
                      z_send.at[k], z_recv.at[k], {"ia": iz ^ k})

    def x_copy(k, m, owner):
        part = aux.at[chunk(owner), slot(k)]
        return remote(part, part, x_send.at[k, m], x_recv.at[k, m],
                      {"ja": ij ^ (CORES * m)})

    def s_copy(k, m, owner):
        part = aux.at[chunk(owner), slot(k)]
        return remote(part, part, s_send.at[k, m], s_recv.at[k, m], {"ja": sibling})

    def p_copy(m):
        return remote(plat.at[chunk(ij ^ m)], lat_in.at[m], p_send.at[m], p_recv.at[m],
                      {"ja": ij ^ m})

    def l_copy(m, owner):
        return remote(lat.at[chunk(owner)], lat.at[chunk(owner)], l_send.at[m],
                      l_recv.at[m], {"ja": ij ^ m})

    load_aux.wait()
    for k in range(1, n):
        z_copy(k).start()

    load_d.wait()
    load_u.wait()

    total = jnp.zeros(plat.shape, F32)
    for j in range(pairs_j):
        total += jnp.dot(d[j], u[j], preferred_element_type=F32)
    plat[...] = total.astype(BF16)

    def halfway(k, place):
        factor = aux[:, k * width:(k + 1) * width]

        @pl.loop(0, n_jp)
        def _(jp):
            for t in range(grp_j):
                block = lax.dot_general(d[jp * grp_j + t], factor, NT,
                                        preferred_element_type=F32)
                half[jp, place * width:(place + 1) * width,
                     t * width:(t + 1) * width] = block.astype(BF16)

    halfway(0, 0)
    for m in range(1, nj):
        p_copy(m).start()

    def pass_on(k):
        z_copy(k).wait_recv()
        for m in range(1, nx):
            x_copy(k, m, ij).start()
        s_copy(k, 0, ij).start()

    def gather_latent():
        mine = plat[chunk(ij), :].astype(F32)
        for m in range(1, nj):
            p_copy(m).wait_recv()
            mine += lat_in[m].astype(F32)
        lat[chunk(ij), :] = mine.astype(BF16)

    def send_latent():
        for m in range(1, nj):
            l_copy(m, ij).start()

    def ladder(first, count, last):
        @pl.loop(0, n_jp)
        def _(jp):
            res = jnp.dot(aux[:, first * width:(first + count) * width],
                          half[jp, :count * width, :], preferred_element_type=F32)
            if first > 0:
                res += acc[jp]
            if not last:
                acc[jp] = res
            else:
                for t in range(grp_j):
                    j = jp * grp_j + t
                    cyc = lax.dot_general(lat[...], u[j], NT, preferred_element_type=F32)
                    out[j] = (res[:, t * width:(t + 1) * width] + cyc).astype(BF16)
                    pltpu.make_async_copy(out.at[j], out_hbm.at[0, j], out_sem.at[j]).start()

    def latent_all():
        for m in range(1, nj):
            l_copy(m, ij ^ m).wait_recv()

    if n > 1:
        pass_on(1)
    gather_latent()
    if n == 1:
        send_latent()
        latent_all()
        ladder(0, 1, True)
    for k in range(1, n):
        if k + 1 < n:
            pass_on(k + 1)
        if k == 1:
            send_latent()
        for m in range(1, nx):
            x_copy(k, m, ij ^ (CORES * m)).wait_recv()
            s_copy(k, m, ij ^ (CORES * m)).start()
        for m in range(nx):
            s_copy(k, m, sibling ^ (CORES * m)).wait_recv()
        halfway(k, k % 2)
        if k == n - 1:
            latent_all()
        if k % 2 == 1:
            ladder(k - 1, 2, k == n - 1)
        elif k == n - 1:
            ladder(k, 1, True)

    for j in range(pairs_j):
        pltpu.make_async_copy(out.at[j], out_hbm.at[0, j], out_sem.at[j]).wait()
    for k in range(1, n):
        z_copy(k).wait_send()
        for m in range(1, nx):
            x_copy(k, m, ij).wait_send()
        for m in range(nx):
            s_copy(k, m, ij ^ (CORES * m)).wait_send()
    for m in range(1, nj):
        p_copy(m).wait_send()
        l_copy(m, ij).wait_send()


def shards(n, nj, doubles, aux_factors, cycle_factors):
    _, pairs_j, width, _ = doubles.shape
    rank = cycle_factors.shape[2]
    grp_j = 2 if pairs_j % 2 == 0 else 1
    nx = nj // CORES
    dma = pltpu.SemaphoreType.DMA
    hbm = pl.BlockSpec(memory_space=pltpu.HBM)
    flops = 4 * n * pairs_j * width**3 + 4 * pairs_j * width * width * rank
    return pl.pallas_call(
        functools.partial(sigma_kernel, n, nj),
        out_shape=jax.ShapeDtypeStruct(doubles.shape, BF16),
        in_specs=[hbm] * 3,
        out_specs=hbm,
        scratch_shapes=[
            pltpu.VMEM((pairs_j, width, width), BF16),
            pltpu.VMEM((pairs_j, width, rank), BF16),
            pltpu.VMEM((width, n * width), BF16),
            pltpu.VMEM((pairs_j // grp_j, 2 * width, grp_j * width), BF16),
            pltpu.VMEM((pairs_j // grp_j, width, grp_j * width), F32),
            pltpu.VMEM((pairs_j, width, width), BF16),
            pltpu.VMEM((width, rank), BF16),
            pltpu.VMEM((nj, width // nj, rank), BF16),
            pltpu.VMEM((width, rank), BF16),
            dma((3,)),
            dma((pairs_j,)),
            dma((n,)), dma((n,)),
            dma((n, nx)), dma((n, nx)),
            dma((n, nx)), dma((n, nx)),
            dma((nj,)), dma((nj,)),
            dma((nj,)), dma((nj,)),
        ],
        compiler_params=pltpu.CompilerParams(
            collective_id=0, has_side_effects=True, vmem_limit_bytes=56 * 2**20),
        cost_estimate=pl.CostEstimate(
            flops=flops, bytes_accessed=4 * doubles.size, transcendentals=0),
    )(doubles, aux_factors, cycle_factors)


def solution(mesh):
    in_specs = (P(("grp", "ia"), "ja", None, None), P("ia", None, None), P())
    out_specs = P(("grp", "ia"), "ja", None, None)
    body = functools.partial(shards, mesh.shape["ia"], mesh.shape["ja"])
    return jax.shard_map(body, mesh=mesh, in_specs=in_specs, out_specs=out_specs, check_vma=False)
```

```python
import functools

import jax
import jax.numpy as jnp
from jax import lax
from jax.experimental import pallas as pl
from jax.experimental.pallas import tpu as pltpu
from jax.sharding import PartitionSpec as P

MESH = pl.DeviceIdType.MESH
F32 = jnp.float32
BF16 = jnp.bfloat16
NT = (((1,), (1,)), ((), ()))
CORES = 2


def sigma_kernel(n, nj, ny, d_hbm, aux_hbm, u_hbm, out, d, u, aux, half, acc,
                 plat, lat_in, lat, load_sem, z_send, z_recv, x_send, x_recv,
                 s_send, s_recv, p_send, p_recv, l_send, l_recv):
    nx = nj // CORES
    pairs_j, width = d.shape[0], d.shape[1]
    grp_j = half.shape[2] // width
    n_jp = pairs_j // grp_j
    rows = width // (ny * nj)
    lat_rows = width // nj
    iz = lax.axis_index("ia")
    iy = lax.axis_index("grp") if ny > 1 else 0
    ij = lax.axis_index("ja")
    sibling = ij ^ 1

    def chunk(owner):
        return pl.ds(pl.multiple_of(owner * rows, rows), rows)

    def lat_chunk(owner):
        return pl.ds(pl.multiple_of(owner * lat_rows, lat_rows), lat_rows)

    def piece(m, base):
        return chunk((iy ^ (m // nx)) * nj + (base ^ (CORES * (m % nx))))

    def slot(k):
        return pl.ds(k * width, width)

    load_aux = pltpu.make_async_copy(aux_hbm.at[0], aux.at[:, slot(0)], load_sem.at[0])
    load_d = pltpu.make_async_copy(d_hbm.at[0], d, load_sem.at[1])
    load_u = pltpu.make_async_copy(
        u_hbm.at[pl.ds(ij * pairs_j, pairs_j)], u, load_sem.at[2])
    load_aux.start()
    load_d.start()
    load_u.start()

    def plane(m):
        where = {"ja": ij ^ (CORES * (m % nx))}
        if m >= nx:
            where["grp"] = iy ^ (m // nx)
        return where

    barrier = pltpu.get_barrier_semaphore()
    for k in range(1, n):
        pl.semaphore_signal(barrier, inc=1, device_id={"ia": iz ^ k}, device_id_type=MESH)
    for m in range(1, nj):
        pl.semaphore_signal(barrier, inc=1, device_id={"ja": ij ^ m}, device_id_type=MESH)
    for m in range(nx, ny * nx):
        pl.semaphore_signal(barrier, inc=1, device_id=plane(m), device_id_type=MESH)
    pl.semaphore_wait(barrier, n - 1 + nj - 1 + (ny - 1) * nx)

    def remote(src, dst, send, recv, where):
        return pltpu.make_async_remote_copy(
            src_ref=src, dst_ref=dst, send_sem=send, recv_sem=recv,
            device_id=where, device_id_type=MESH)

    def z_copy(k):
        return remote(aux.at[piece(0, ij), slot(0)], aux.at[piece(0, ij), slot(k)],
                      z_send.at[k], z_recv.at[k], {"ia": iz ^ k})

    def x_copy(k, m, from_m=0):
        part = aux.at[piece(from_m, ij), slot(k)]
        return remote(part, part, x_send.at[k, m], x_recv.at[k, m], plane(m))

    def s_copy(k, m, base):
        part = aux.at[piece(m, base), slot(k)]
        return remote(part, part, s_send.at[k, m], s_recv.at[k, m], {"ja": sibling})

    def p_copy(m):
        return remote(plat.at[lat_chunk(ij ^ m)], lat_in.at[m], p_send.at[m], p_recv.at[m],
                      {"ja": ij ^ m})

    def l_copy(m, owner):
        return remote(lat.at[lat_chunk(owner)], lat.at[lat_chunk(owner)], l_send.at[m],
                      l_recv.at[m], {"ja": ij ^ m})

    load_aux.wait()
    for k in range(1, n):
        z_copy(k).start()

    load_d.wait()
    load_u.wait()

    total = jnp.zeros(plat.shape, F32)
    for j in range(pairs_j):
        total += jnp.dot(d[j], u[j], preferred_element_type=F32)
    plat[...] = total.astype(BF16)

    def halfway(k, place):
        factor = aux[:, k * width:(k + 1) * width]

        @pl.loop(0, n_jp)
        def _(jp):
            for t in range(grp_j):
                block = lax.dot_general(d[jp * grp_j + t], factor, NT,
                                        preferred_element_type=F32)
                half[jp, place * width:(place + 1) * width,
                     t * width:(t + 1) * width] = block.astype(BF16)

    halfway(0, 0)
    for m in range(1, nj):
        p_copy(m).start()

    passed, relayed = set(), set()

    def pass_on(k):
        if k >= n or k in passed:
            return
        passed.add(k)
        z_copy(k).wait_recv()
        for m in range(1, ny * nx):
            x_copy(k, m).start()
        s_copy(k, 0, ij).start()

    def relay(k):
        if k >= n or k in relayed:
            return
        relayed.add(k)
        for m in range(1, ny * nx):
            x_copy(k, m, m).wait_recv()
            s_copy(k, m, ij).start()

    def gather_latent():
        mine = plat[lat_chunk(ij), :].astype(F32)
        for m in range(1, nj):
            p_copy(m).wait_recv()
            mine += lat_in[m].astype(F32)
        lat[lat_chunk(ij), :] = mine.astype(BF16)

    def send_latent():
        for m in range(1, nj):
            l_copy(m, ij).start()

    def ladder(first, count, last):
        @pl.loop(0, n_jp)
        def _(jp):
            res = jnp.dot(aux[:, first * width:(first + count) * width],
                          half[jp, :count * width, :], preferred_element_type=F32)
            if first > 0:
                res += acc[jp]
            if not last:
                acc[jp] = res
            else:
                for t in range(grp_j):
                    j = jp * grp_j + t
                    cyc = lax.dot_general(lat[...], u[j], NT, preferred_element_type=F32)
                    out[0, j] = (res[:, t * width:(t + 1) * width] + cyc).astype(BF16)

    def latent_all():
        for m in range(1, nj):
            l_copy(m, ij ^ m).wait_recv()

    pass_on(1)
    pass_on(2)
    gather_latent()
    relay(1)
    pass_on(3)
    send_latent()
    if n == 1:
        latent_all()
        ladder(0, 1, True)
    for k in range(1, n):
        for m in range(ny * nx):
            s_copy(k, m, sibling).wait_recv()
        halfway(k, k % 2)
        relay(k + 1)
        pass_on(k + 3)
        if k == n - 1:
            latent_all()
        if k % 2 == 1:
            relay(k + 2)
            ladder(k - 1, 2, k == n - 1)
        elif k == n - 1:
            ladder(k, 1, True)

    for k in range(1, n):
        z_copy(k).wait_send()
        for m in range(1, ny * nx):
            x_copy(k, m).wait_send()
        for m in range(ny * nx):
            s_copy(k, m, ij).wait_send()
    for m in range(1, nj):
        p_copy(m).wait_send()
        l_copy(m, ij).wait_send()


def shards(n, nj, grps, doubles, aux_factors, cycle_factors):
    _, pairs_j, width, _ = doubles.shape
    rank = cycle_factors.shape[2]
    grp_j = 2 if pairs_j % 2 == 0 else 1
    ny = grps if width % (grps * nj * 16) == 0 else 1
    nx = nj // CORES * ny
    dma = pltpu.SemaphoreType.DMA
    hbm = pl.BlockSpec(memory_space=pltpu.HBM)
    flops = 4 * n * pairs_j * width**3 + 4 * pairs_j * width * width * rank
    return pl.pallas_call(
        functools.partial(sigma_kernel, n, nj, ny),
        out_shape=pltpu.VMEM(doubles.shape, BF16),
        in_specs=[hbm] * 3,
        out_specs=pl.BlockSpec(memory_space=pltpu.VMEM),
        scratch_shapes=[
            pltpu.VMEM((pairs_j, width, width), BF16),
            pltpu.VMEM((pairs_j, width, rank), BF16),
            pltpu.VMEM((width, n * width), BF16),
            pltpu.VMEM((pairs_j // grp_j, 2 * width, grp_j * width), BF16),
            pltpu.VMEM((pairs_j // grp_j, width, grp_j * width), F32),
            pltpu.VMEM((width, rank), BF16),
            pltpu.VMEM((nj, width // nj, rank), BF16),
            pltpu.VMEM((width, rank), BF16),
            dma((3,)),
            dma((n,)), dma((n,)),
            dma((n, nx)), dma((n, nx)),
            dma((n, nx)), dma((n, nx)),
            dma((nj,)), dma((nj,)),
            dma((nj,)), dma((nj,)),
        ],
        compiler_params=pltpu.CompilerParams(
            collective_id=0, has_side_effects=True, vmem_limit_bytes=67043328 - doubles.size * 2 - 2**16),
        cost_estimate=pl.CostEstimate(
            flops=flops, bytes_accessed=4 * doubles.size, transcendentals=0),
    )(doubles, aux_factors, cycle_factors)


def solution(mesh):
    in_specs = (P(("grp", "ia"), "ja", None, None), P("ia", None, None), P())
    out_specs = P(("grp", "ia"), "ja", None, None)
    body = functools.partial(shards, mesh.shape["ia"], mesh.shape["ja"], mesh.shape["grp"])
    return jax.shard_map(body, mesh=mesh, in_specs=in_specs, out_specs=out_specs, check_vma=False)
```
